32 devices in a mesh: img: 8 (over z, x), row: 4 (over y, core).
Axes of the slice: x: 2, y: 2, z: 4, core: 2. Of those that a mesh axis runs over, the one named last changes fastest.
Arguments:
- tokens: bfloat16 [8, 32, 128, 1024], P('img', 'row'), may hold values from -14 to 14
- proj_weight: bfloat16 [1024, 256], replicated, may hold values from -0.1875 to 0.1875
- proj_bias: float32 [256], replicated, may hold values from -3 to 3
- conv_weight: bfloat16 [4, 3, 3, 256, 256], replicated, may hold values from -0.125 to 0.125
- bn_gain: float32 [4, 256], replicated, may hold values from 0.1 to 1.9
- bn_bias: float32 [4, 256], replicated, may hold values from -3 to 3
Outputs:
- joining_out: bfloat16 [8, 32, 128, 256], P('img', 'row')
The draws below stay inside these ranges and needn't reach their ends.
All inputs are finite; a program needn't handle non-finite values.
Results may differ from the reference program's by a relative error of at most 0.0071.
Values may be sent and summed in bfloat16 or wider, within the bound.
A program may use at most 64 MiB of HBM per device.

```python
import math
import jax
import jax.numpy as jnp
from jax import lax

EMBED = 1024
FW = 256
COLS = 128
IMAGES = 8
HEIGHT = 32


def draw_tokens(key, part):
    key_image, key_row, key_base = jax.random.split(key, 3)
    image_scale = jnp.exp(jax.random.uniform(key_image, (IMAGES, 1, 1, 1), jnp.float32, 0.0, math.log(4.0)))
    row_scale = jnp.exp(jax.random.uniform(key_row, (1, HEIGHT, 1, 1), jnp.float32, 0.0, math.log(2.5)))
    base = jnp.clip(jax.random.normal(key_base, (IMAGES, HEIGHT, COLS, EMBED), jnp.float32), -4.0, 4.0)
    return (base * image_scale * row_scale / 3.0).astype(jnp.bfloat16)


def centred(key, dims, deviation, most, kind=jnp.bfloat16):
    return jnp.clip(deviation * jax.random.normal(key, dims, jnp.float32), -most, most).astype(kind)


def setup_inputs(seed: int = 0) -> dict:
    key_of = jax.random.split(jax.random.key(seed), 7)
    tokens = draw_tokens(jax.random.fold_in(key_of[6], 71), 0)
    proj_weight = centred(key_of[1], (EMBED, FW), EMBED ** -0.5, 0.1875)
    proj_bias = centred(key_of[2], (FW,), 0.5, 3.0, jnp.float32)
    conv_weight = centred(key_of[3], (4, 3, 3, FW, FW), (9 * FW) ** -0.5, 0.125)
    bn_gain = jnp.clip(1.0 + 0.18 * jax.random.normal(key_of[4], (4, FW), jnp.float32), 0.1, 1.9)
    bn_bias = centred(key_of[5], (4, FW), 0.5, 3.0, jnp.float32)
    return {"tokens": tokens, "proj_weight": proj_weight, "proj_bias": proj_bias, "conv_weight": conv_weight, "bn_gain": bn_gain, "bn_bias": bn_bias}


epsilon = 1e-05

def conv_three(source, kernel):
    return lax.conv_general_dilated(source.astype(jnp.float32), kernel.astype(jnp.float32), (1, 1), ((1, 1), (1, 1)), dimension_numbers=('NHWC', 'HWIO', 'NHWC'), precision=lax.Precision.HIGHEST)

def batch_norm(conv_out, gain_row, shift_row):
    average = lax.optimization_barrier(jnp.mean(conv_out, axis=(0, 1, 2)))
    spread = lax.optimization_barrier(jnp.mean(jnp.square(conv_out - average), axis=(0, 1, 2)))
    return (conv_out - average) * lax.rsqrt(spread + epsilon) * gain_row + shift_row

def residual_unit(source, conv_weight, bn_gain, bn_bias, first):
    active = jax.nn.relu(source)
    conv_first = conv_three(active, conv_weight[first])
    hidden = jax.nn.relu(batch_norm(conv_first, bn_gain[first], bn_bias[first])).astype(jnp.bfloat16)
    conv_second = conv_three(hidden, conv_weight[first + 1])
    return source.astype(jnp.float32) + batch_norm(conv_second, bn_gain[first + 1], bn_bias[first + 1])

def reference(tokens, proj_weight, proj_bias, conv_weight, bn_gain, bn_bias):
    img_count, row_count, col_count, embed_dim = tokens.shape
    flat = jnp.dot(tokens.reshape(-1, embed_dim), proj_weight, preferred_element_type=jnp.float32) + proj_bias
    feature = flat.astype(jnp.bfloat16).reshape(img_count, row_count, col_count, -1)
    joined = residual_unit(feature, conv_weight, bn_gain, bn_bias, 0).astype(jnp.bfloat16)
    return residual_unit(joined, conv_weight, bn_gain, bn_bias, 2).astype(jnp.bfloat16)
```

```python
import functools

import jax
import jax.numpy as jnp
from jax import lax
from jax.experimental import pallas as pl
from jax.experimental.pallas import tpu as pltpu
from jax.sharding import PartitionSpec as P

epsilon = 1e-05
LOGICAL = pl.DeviceIdType.LOGICAL
F32 = jnp.float32
BF16 = jnp.bfloat16
STEP = 2
UNROLL = 63
VMEM_LIMIT = 40 * 1024 * 1024


def kernel(
    imgs,
    strips,
    height,
    cols,
    tokens_ref,
    pw_ref,
    pb_ref,
    cw_ref,
    gain_ref,
    bias_ref,
    out_ref,
    tok,
    pw,
    pb,
    cw,
    gain,
    bias,
    feat,
    joined,
    xcat,
    raw,
    rim_out,
    rim_in,
    stats,
    peers,
    load_sem,
    weight_sem,
    halo_send,
    halo_recv,
    stat_send,
    stat_recv,
):
    count = imgs * strips
    width = feat.shape[-1]
    cells = height * cols
    me_row = lax.axis_index("row")
    me = lax.axis_index("img") * strips + me_row
    has_up, has_down = me_row > 0, me_row < strips - 1
    above = me - jnp.where(has_up, 1, 0)
    below = me + jnp.where(has_down, 1, 0)

    def peer(distance):
        target = me + distance
        return jnp.where(target >= count, target - count, target)

    def rows(first, number):
        return pl.ds(first * cols, number * cols)

    loads = [
        pltpu.make_async_copy(pw_ref, pw, load_sem.at[0]),
        pltpu.make_async_copy(tokens_ref.at[rows(0, 1)], tok.at[rows(0, 1)], load_sem.at[1]),
        pltpu.make_async_copy(
            tokens_ref.at[rows(height - 1, 1)], tok.at[rows(1, 1)], load_sem.at[2]
        ),
        pltpu.make_async_copy(pb_ref, pb, load_sem.at[3]),
        pltpu.make_async_copy(
            tokens_ref.at[rows(1, height - 2)], tok.at[rows(2, height - 2)], load_sem.at[4]
        ),
        pltpu.make_async_copy(gain_ref, gain, load_sem.at[5]),
        pltpu.make_async_copy(bias_ref, bias, load_sem.at[6]),
    ]
    weights = [
        pltpu.make_async_copy(
            cw_ref.at[pl.ds(3 * k, 3)], cw.at[pl.ds(3 * k, 3)], weight_sem.at[k]
        )
        for k in range(4)
    ]
    for load in loads[:5]:
        load.start()

    barrier = pltpu.get_barrier_semaphore()

    @pl.loop(1, count)
    def _(distance):
        pl.semaphore_signal(
            barrier, inc=1, device_id=peer(distance), device_id_type=LOGICAL
        )

    for weight in weights:
        weight.start()
    for load in loads[5:]:
        load.start()

    @pl.when(jnp.logical_not(has_up))
    def _():
        feat[rows(0, 1), :] = jnp.zeros((cols, width), BF16)
        for k in range(3):
            rim_in[k, 0] = jnp.zeros((cols, width), BF16)

    @pl.when(jnp.logical_not(has_down))
    def _():
        feat[rows(height + 1, 1), :] = jnp.zeros((cols, width), BF16)
        for k in range(3):
            rim_in[k, 1] = jnp.zeros((cols, width), BF16)

    column = lax.broadcasted_iota(jnp.int32, (cols, width), 0)
    at_left, at_right = column == 0, column == cols - 1

    def put(row, value):
        at = rows(row, 1)
        xcat[at, 0:width] = jnp.where(at_left, 0.0, pltpu.roll(value, 1, 0)).astype(BF16)
        xcat[at, width : 2 * width] = value.astype(BF16)
        xcat[at, 2 * width : 3 * width] = jnp.where(
            at_right, 0.0, pltpu.roll(value, cols - 1, 0)
        ).astype(BF16)

    def project(slot, number, where):
        value = jnp.dot(tok[rows(slot, number), :], pw[...], preferred_element_type=F32)
        value = (value + pb[...]).astype(BF16)
        for i, row in enumerate(where):
            part = value[i * cols : (i + 1) * cols]
            feat[rows(row + 1, 1), :] = part
            put(row + 1, jnp.maximum(part.astype(F32), 0.0))

    def halo(phase, up_from, up_to, down_from, down_to):
        up = pltpu.make_async_remote_copy(
            src_ref=up_from,
            dst_ref=up_to,
            send_sem=halo_send.at[phase, 0],
            recv_sem=halo_recv.at[phase, 1],
            device_id=above,
            device_id_type=LOGICAL,
        )
        down = pltpu.make_async_remote_copy(
            src_ref=down_from,
            dst_ref=down_to,
            send_sem=halo_send.at[phase, 1],
            recv_sem=halo_recv.at[phase, 0],
            device_id=below,
            device_id_type=LOGICAL,
        )
        return up, down

    def feature_halo():
        return halo(
            0,
            feat.at[rows(1, 1)],
            feat.at[rows(height + 1, 1)],
            feat.at[rows(height, 1)],
            feat.at[rows(0, 1)],
        )

    def raw_halo(k):
        return halo(
            k + 1, rim_out.at[k, 0], rim_in.at[k, 1], rim_out.at[k, 1], rim_in.at[k, 0]
        )

    def send_halo(pair):
        up, down = pair

        @pl.when(has_up)
        def _():
            up.start()

        @pl.when(has_down)
        def _():
            down.start()

    def take_halo(pair):
        up, down = pair

        @pl.when(has_up)
        def _():
            down.wait_recv()

        @pl.when(has_down)
        def _():
            up.wait_recv()

    def end_halo(pair):
        up, down = pair

        @pl.when(has_up)
        def _():
            up.wait_send()

        @pl.when(has_down)
        def _():
            down.wait_send()

    def taps(k, first, number, which):
        return sum(
            jnp.dot(xcat[rows(first + dy, number), :], cw[3 * k + dy], preferred_element_type=F32)
            for dy in which
        )

    def fold(value):
        return jnp.sum(value.reshape(value.shape[0] // 8, 8, width), axis=0)

    class Moments:
        def add(self, value):
            if not hasattr(self, "pivot"):
                self.pivot = jnp.sum(fold(value), axis=0, keepdims=True) / value.shape[0]
                self.first = jnp.zeros((8, width), F32)
                self.second = jnp.zeros((8, width), F32)
            gap = value - self.pivot
            self.first += fold(gap)
            self.second += fold(jnp.square(gap))

        def total(self):
            first = jnp.sum(self.first, axis=0, keepdims=True)
            second = jnp.sum(self.second, axis=0, keepdims=True)
            return first + cells * self.pivot, second - jnp.square(first) / cells

    def stat_copy(k, distance):
        return pltpu.make_async_remote_copy(
            src_ref=stats.at[k],
            dst_ref=peers.at[k, distance - 1],
            send_sem=stat_send.at[k],
            recv_sem=stat_recv.at[k],
            device_id=peer(distance),
            device_id_type=LOGICAL,
        )

    def send_stat(k, moments):
        total, squares = moments.total()
        stats[k] = jnp.concatenate([total, squares], axis=0)
        if count - 1 <= UNROLL:
            for distance in range(1, count):
                stat_copy(k, distance).start()
        else:
            pl.loop(1, count)(lambda distance: stat_copy(k, distance).start())

    def take_stat(k):
        own = stats[k]
        pltpu.make_async_copy(peers.at[k], peers.at[k], stat_recv.at[k]).wait()
        every = peers[k]
        total = jnp.sum(every, axis=0) + own
        even = total[0:1] / count
        gaps = jnp.sum(jnp.square(every[:, 0, :] - even), axis=0, keepdims=True)
        gaps += jnp.square(own[0:1] - even)
        squares = total[1:2] + gaps / cells
        size = cells * count
        average = total[0:1] / size
        scale = lax.rsqrt(squares / size + epsilon) * gain[k : k + 1, :]
        return average, scale, bias[k : k + 1, :]

    def normed(k, row, norm):
        average, scale, shift = norm
        if row == 0:
            value = rim_in[k, 0].astype(F32)
        elif row == height + 1:
            value = rim_in[k, 1].astype(F32)
        else:
            value = raw[k, rows(row - 1, 1), :]
        return (value - average) * scale + shift

    def inside(row, value):
        if row == 0:
            return jnp.where(has_up, value, 0.0)
        if row == height + 1:
            return jnp.where(has_down, value, 0.0)
        return value

    def conv_stage(k, fill):
        weights[k].wait()
        moments = Moments()
        filled = 0
        for first in range(0, height, STEP):
            while filled < first + STEP + 2:
                fill(filled)
                filled += 1
            value = taps(k, first, STEP, range(3))
            raw[k, rows(first, STEP), :] = value
            if k < 3 and first == 0:
                rim_out[k, 0] = value[:cols].astype(BF16)
            if k < 3 and first + STEP == height:
                rim_out[k, 1] = value[-cols:].astype(BF16)
            moments.add(value)
        send_stat(k, moments)
        if k < 3:
            send_halo(raw_halo(k))

    loads[0].wait()
    loads[1].wait()
    loads[2].wait()
    loads[3].wait()
    project(0, 2, (0, height - 1))
    pl.semaphore_wait(barrier, count - 1)
    send_halo(feature_halo())
    loads[4].wait()
    for slot in range(2, height, 2):
        project(slot, 2, (slot - 1, slot))

    weights[0].wait()
    moments = Moments()
    for first in range(1, height - 1, 2):
        value = taps(0, first, 2, range(3))
        raw[0, rows(first, 2), :] = value
        moments.add(value)
    top = taps(0, 0, 1, (1, 2))
    bottom = taps(0, height - 1, 1, (0, 1))
    raw[0, rows(0, 1), :] = top
    raw[0, rows(height - 1, 1), :] = bottom
    take_halo(feature_halo())
    put(0, jnp.maximum(feat[rows(0, 1), :].astype(F32), 0.0))
    put(height + 1, jnp.maximum(feat[rows(height + 1, 1), :].astype(F32), 0.0))
    top = raw[0, rows(0, 1), :] + taps(0, 0, 1, (0,))
    bottom = raw[0, rows(height - 1, 1), :] + taps(0, height - 1, 1, (2,))
    for side, row, value in ((0, 0, top), (1, height - 1, bottom)):
        raw[0, rows(row, 1), :] = value
        rim_out[0, side] = value.astype(BF16)
        moments.add(value)
    send_stat(0, moments)
    send_halo(raw_halo(0))
    loads[5].wait()
    loads[6].wait()

    def hidden(k):
        norm = take_stat(k)
        take_halo(raw_halo(k))

        def fill(row):
            put(row, inside(row, jnp.maximum(normed(k, row, norm), 0.0)))

        return fill

    conv_stage(1, hidden(0))

    norm_1 = take_stat(1)
    take_halo(raw_halo(1))

    def join(row):
        value = (feat[rows(row, 1), :].astype(F32) + normed(1, row, norm_1)).astype(BF16)
        if 1 <= row <= height:
            joined[rows(row - 1, 1), :] = value
        put(row, inside(row, jnp.maximum(value.astype(F32), 0.0)))

    conv_stage(2, join)
    conv_stage(3, hidden(2))
    norm_3 = take_stat(3)

    for row in range(height):
        value = joined[rows(row, 1), :].astype(F32) + normed(3, row + 1, norm_3)
        out_ref[rows(row, 1), :] = value.astype(BF16)

    end_halo(feature_halo())
    for k in range(3):
        end_halo(raw_halo(k))
    for k in range(4):
        pltpu.make_async_copy(peers.at[k], peers.at[k], stat_send.at[k]).wait()


def solution(mesh):
    imgs, strips = mesh.shape["img"], mesh.shape["row"]

    def on_device(tokens, proj_weight, proj_bias, conv_weight, bn_gain, bn_bias):
        images, height, cols, embed = tokens.shape
        convs, taps, _, width, _ = conv_weight.shape
        assert images == 1 and height % 2 == 0 and height >= 4
        count = imgs * strips
        cells = height * cols
        hbm = pl.BlockSpec(memory_space=pltpu.HBM)
        vmem = pl.BlockSpec(memory_space=pltpu.VMEM)
        operands = [
            tokens.reshape(cells, embed),
            proj_weight,
            proj_bias.reshape(1, width),
            conv_weight.reshape(convs * taps, taps * width, width),
            bn_gain,
            bn_bias,
        ]
        out = pl.pallas_call(
            functools.partial(kernel, imgs, strips, height, cols),
            out_shape=pltpu.VMEM((cells, width), BF16),
            in_specs=[hbm] * 6,
            out_specs=vmem,
            scratch_shapes=[
                pltpu.VMEM((cells, embed), BF16),
                pltpu.VMEM((embed, width), BF16),
                pltpu.VMEM((1, width), F32),
                pltpu.VMEM((convs * taps, taps * width, width), BF16),
                pltpu.VMEM((convs, width), F32),
                pltpu.VMEM((convs, width), F32),
                pltpu.VMEM((cells + 2 * cols, width), BF16),
                pltpu.VMEM((cells, width), BF16),
                pltpu.VMEM((cells + 2 * cols, taps * width), BF16),
                pltpu.VMEM((convs, cells, width), F32),
                pltpu.VMEM((convs - 1, 2, cols, width), BF16),
                pltpu.VMEM((convs - 1, 2, cols, width), BF16),
                pltpu.VMEM((convs, 2, width), F32),
                pltpu.VMEM((convs, count - 1, 2, width), F32),
                pltpu.SemaphoreType.DMA((7,)),
                pltpu.SemaphoreType.DMA((convs,)),
                pltpu.SemaphoreType.DMA((convs, 2)),
                pltpu.SemaphoreType.DMA((convs, 2)),
                pltpu.SemaphoreType.DMA((convs,)),
                pltpu.SemaphoreType.DMA((convs,)),
            ],
            compiler_params=pltpu.CompilerParams(
                collective_id=0, has_side_effects=True, vmem_limit_bytes=VMEM_LIMIT
            ),
        )(*[pltpu.with_memory_space_constraint(x, pltpu.HBM) for x in operands])
        return out.reshape(images, height, cols, width)

    in_specs = (P("img", "row", None, None), P(), P(), P(), P(), P())
    return jax.shard_map(
        on_device,
        mesh=mesh,
        in_specs=in_specs,
        out_specs=P("img", "row", None, None),
        check_vma=False,
    )
```

```python
import functools

import jax
import jax.numpy as jnp
from jax import lax
from jax.experimental import pallas as pl
from jax.experimental.pallas import tpu as pltpu
from jax.sharding import PartitionSpec as P

epsilon = 1e-05
LOGICAL = pl.DeviceIdType.LOGICAL
F32 = jnp.float32
BF16 = jnp.bfloat16
STEP = 2
UNROLL = 63
VMEM_LIMIT = 40 * 1024 * 1024


def bits_of(count):
    return [2**b for b in range(count.bit_length() - 1)]


def kernel(
    imgs,
    strips,
    height,
    cols,
    tokens_ref,
    pw_ref,
    pb_ref,
    cw_ref,
    gain_ref,
    bias_ref,
    out_ref,
    tok,
    pw,
    pb,
    cw,
    gain,
    bias,
    feat,
    joined,
    xcat,
    raw,
    rim_out,
    rim_in,
    stats,
    peers,
    load_sem,
    weight_sem,
    halo_send,
    halo_recv,
    stat_send,
    stat_recv,
    near,
    everyone,
):
    count = imgs * strips
    width = feat.shape[-1]
    cells = height * cols
    me_row = lax.axis_index("row")
    me = lax.axis_index("img") * strips + me_row
    has_up, has_down = me_row > 0, me_row < strips - 1
    above = me - jnp.where(has_up, 1, 0)
    below = me + jnp.where(has_down, 1, 0)

    flips = [bit - 2 * bit * lax.rem(me // bit, 2) for bit in bits_of(count)]

    def peer(distance):
        if isinstance(distance, int):
            return me + sum(flip for b, flip in enumerate(flips) if distance >> b & 1)
        return me + sum(flip * lax.rem(distance // 2**b, 2) for b, flip in enumerate(flips))

    half = count // 2
    odd = lax.rem(me_row, 2)
    is_odd, is_even = odd == 1, odd == 0
    partner = me + 1 - 2 * odd

    def rows(first, number):
        return pl.ds(first * cols, number * cols)

    loads = [
        pltpu.make_async_copy(pw_ref, pw, load_sem.at[0]),
        pltpu.make_async_copy(tokens_ref.at[rows(0, 1)], tok.at[rows(0, 1)], load_sem.at[1]),
        pltpu.make_async_copy(
            tokens_ref.at[rows(height - 1, 1)], tok.at[rows(1, 1)], load_sem.at[2]
        ),
        pltpu.make_async_copy(pb_ref, pb, load_sem.at[3]),
        pltpu.make_async_copy(
            tokens_ref.at[rows(1, height - 2)], tok.at[rows(2, height - 2)], load_sem.at[4]
        ),
        pltpu.make_async_copy(gain_ref, gain, load_sem.at[5]),
        pltpu.make_async_copy(bias_ref, bias, load_sem.at[6]),
    ]
    weights = [
        pltpu.make_async_copy(
            cw_ref.at[pl.ds(3 * k, 3)], cw.at[pl.ds(3 * k, 3)], weight_sem.at[k]
        )
        for k in range(4)
    ]
    for load in loads[:4]:
        load.start()

    barrier = pltpu.get_barrier_semaphore()

    def greet(device):
        pl.semaphore_signal(barrier, inc=1, device_id=device, device_id_type=LOGICAL)

    @pl.when(is_odd)
    def _():
        greet(partner)

        @pl.when(has_down)
        def _():
            greet(below)

    @pl.when(jnp.logical_and(is_even, me_row >= 2))
    def _():
        greet(me - 2)

    @pl.loop(1, half)
    def _(distance):
        greet(peer(2 * (half - distance)) + 1 - odd)

    @pl.when(is_even)
    def _():
        greet(partner)

    loads[4].start(priority=1)
    for weight in weights:
        weight.start(priority=1)
    for load in loads[5:]:
        load.start(priority=1)

    @pl.when(jnp.logical_not(has_up))
    def _():
        feat[rows(0, 1), :] = jnp.zeros((cols, width), BF16)
        for k in range(3):
            rim_in[k, 0] = jnp.zeros((cols, width), BF16)

    @pl.when(jnp.logical_not(has_down))
    def _():
        feat[rows(height + 1, 1), :] = jnp.zeros((cols, width), BF16)
        for k in range(3):
            rim_in[k, 1] = jnp.zeros((cols, width), BF16)

    column = lax.broadcasted_iota(jnp.int32, (cols, width), 0)
    at_left, at_right = column == 0, column == cols - 1

    def put(row, value):
        at = rows(row, 1)
        xcat[at, 0:width] = jnp.where(at_left, 0.0, pltpu.roll(value, 1, 0)).astype(BF16)
        xcat[at, width : 2 * width] = value.astype(BF16)
        xcat[at, 2 * width : 3 * width] = jnp.where(
            at_right, 0.0, pltpu.roll(value, cols - 1, 0)
        ).astype(BF16)

    def project(slot, number, where):
        value = jnp.dot(tok[rows(slot, number), :], pw[...], preferred_element_type=F32)
        value = (value + pb[...]).astype(BF16)
        for i, row in enumerate(where):
            feat[rows(row + 1, 1), :] = value[i * cols : (i + 1) * cols]

    def activate(row):
        put(row, jnp.maximum(feat[rows(row, 1), :].astype(F32), 0.0))

    def halo(phase, up_from, up_to, down_from, down_to):
        up = pltpu.make_async_remote_copy(
            src_ref=up_from,
            dst_ref=up_to,
            send_sem=halo_send.at[phase, 0],
            recv_sem=halo_recv.at[phase, 1],
            device_id=above,
            device_id_type=LOGICAL,
        )
        down = pltpu.make_async_remote_copy(
            src_ref=down_from,
            dst_ref=down_to,
            send_sem=halo_send.at[phase, 1],
            recv_sem=halo_recv.at[phase, 0],
            device_id=below,
            device_id_type=LOGICAL,
        )
        return up, down

    def feature_halo():
        return halo(
            0,
            feat.at[rows(1, 1)],
            feat.at[rows(height + 1, 1)],
            feat.at[rows(height, 1)],
            feat.at[rows(0, 1)],
        )

    def raw_halo(k):
        return halo(
            k + 1, rim_out.at[k, 0], rim_in.at[k, 1], rim_out.at[k, 1], rim_in.at[k, 0]
        )

    def send_halo(pair):
        up, down = pair

        @pl.when(has_up)
        def _():
            up.start()

        @pl.when(has_down)
        def _():
            down.start()

    def take_halo(pair):
        up, down = pair

        @pl.when(has_up)
        def _():
            down.wait_recv()

        @pl.when(has_down)
        def _():
            up.wait_recv()

    def end_halo(pair):
        up, down = pair

        @pl.when(has_up)
        def _():
            up.wait_send()

        @pl.when(has_down)
        def _():
            down.wait_send()

    def taps(k, first, number, which):
        return sum(
            jnp.dot(xcat[rows(first + dy, number), :], cw[3 * k + dy], preferred_element_type=F32)
            for dy in which
        )

    def fold(value):
        return jnp.sum(value.reshape(value.shape[0] // 8, 8, width), axis=0)

    class Moments:
        def add(self, value):
            if not hasattr(self, "pivot"):
                self.pivot = jnp.sum(fold(value), axis=0, keepdims=True) / value.shape[0]
                self.first = jnp.zeros((8, width), F32)
                self.second = jnp.zeros((8, width), F32)
            gap = value - self.pivot
            self.first += fold(gap)
            self.second += fold(jnp.square(gap))

        def total(self):
            first = jnp.sum(self.first, axis=0, keepdims=True)
            second = jnp.sum(self.second, axis=0, keepdims=True)
            return first + cells * self.pivot, second - jnp.square(first) / cells

    def stat_copy(k, distance):
        return pltpu.make_async_remote_copy(
            src_ref=stats.at[k],
            dst_ref=peers.at[k, distance - 1],
            send_sem=stat_send.at[k],
            recv_sem=stat_recv.at[k],
            device_id=peer(distance),
            device_id_type=LOGICAL,
        )

    def send_stat(k, moments):
        total, squares = moments.total()
        stats[k] = jnp.concatenate([total, squares], axis=0)
        if count - 1 <= UNROLL:
            for distance in range(count - 1, 0, -1):
                stat_copy(k, distance).start()
        else:
            pl.loop(1, count)(lambda distance: stat_copy(k, count - distance).start())

    def take_stat(k):
        own = stats[k]
        pltpu.make_async_copy(peers.at[k], peers.at[k], stat_recv.at[k]).wait()
        every = peers[k]
        total = jnp.sum(every, axis=0) + own
        even = total[0:1] / count
        gaps = jnp.sum(jnp.square(every[:, 0, :] - even), axis=0, keepdims=True)
        gaps += jnp.square(own[0:1] - even)
        squares = total[1:2] + gaps / cells
        size = cells * count
        average = total[0:1] / size
        scale = lax.rsqrt(squares / size + epsilon) * gain[k : k + 1, :]
        return average, scale, bias[k : k + 1, :]

    def normed(k, row, norm):
        average, scale, shift = norm
        if row == 0:
            value = rim_in[k, 0].astype(F32)
        elif row == height + 1:
            value = rim_in[k, 1].astype(F32)
        else:
            value = raw[k, rows(row - 1, 1), :]
        return (value - average) * scale + shift

    def inside(row, value):
        if row == 0:
            return jnp.where(has_up, value, 0.0)
        if row == height + 1:
            return jnp.where(has_down, value, 0.0)
        return value

    def conv_stage(k, fill):
        weights[k].wait()
        moments = Moments()
        filled = 0
        for first in range(0, height, STEP):
            while filled < first + STEP + 2:
                fill(filled)
                filled += 1
            value = taps(k, first, STEP, range(3))
            raw[k, rows(first, STEP), :] = value
            if k < 3 and first == 0:
                rim_out[k, 0] = value[:cols].astype(BF16)
            if k < 3 and first + STEP == height:
                rim_out[k, 1] = value[-cols:].astype(BF16)
            moments.add(value)
        send_stat(k, moments)
        if k < 3:
            send_halo(raw_halo(k))

    loads[0].wait()
    loads[1].wait()
    loads[2].wait()
    loads[3].wait()
    project(0, 2, (0, height - 1))

    @pl.when(is_even)
    def _():
        beside = jnp.where(me_row >= 2, 1, 0) + jnp.where(me_row + 2 < strips, 1, 0)
        pl.semaphore_wait(barrier, 1 + beside)
        pl.semaphore_signal(near, inc=1, device_id=partner, device_id_type=LOGICAL)

    @pl.when(is_odd)
    def _():
        pl.semaphore_wait(near, 1)

    send_halo(feature_halo())
    loads[4].wait()
    activate(1)
    activate(height)
    for slot in range(2, height, 2):
        project(slot, 2, (slot - 1, slot))
        activate(slot)
        activate(slot + 1)

    weights[0].wait()
    moments = Moments()
    for first in range(1, height - 1, 2):
        value = taps(0, first, 2, range(3))
        raw[0, rows(first, 2), :] = value
        moments.add(value)
    top = taps(0, 0, 1, (1, 2))
    bottom = taps(0, height - 1, 1, (0, 1))
    raw[0, rows(0, 1), :] = top
    raw[0, rows(height - 1, 1), :] = bottom
    take_halo(feature_halo())
    activate(0)
    activate(height + 1)
    top = raw[0, rows(0, 1), :] + taps(0, 0, 1, (0,))
    bottom = raw[0, rows(height - 1, 1), :] + taps(0, height - 1, 1, (2,))
    for side, row, value in ((0, 0, top), (1, height - 1, bottom)):
        raw[0, rows(row, 1), :] = value
        rim_out[0, side] = value.astype(BF16)
        moments.add(value)

    @pl.when(is_odd)
    def _():
        pl.semaphore_wait(barrier, count - 1)
        pl.semaphore_signal(everyone, inc=1, device_id=partner, device_id_type=LOGICAL)

    @pl.when(is_even)
    def _():
        pl.semaphore_wait(everyone, 1)

    send_stat(0, moments)
    send_halo(raw_halo(0))
    loads[5].wait()
    loads[6].wait()

    def hidden(k):
        norm = take_stat(k)
        take_halo(raw_halo(k))

        def fill(row):
            put(row, inside(row, jnp.maximum(normed(k, row, norm), 0.0)))

        return fill

    conv_stage(1, hidden(0))

    norm_1 = take_stat(1)
    take_halo(raw_halo(1))

    def join(row):
        value = (feat[rows(row, 1), :].astype(F32) + normed(1, row, norm_1)).astype(BF16)
        if 1 <= row <= height:
            joined[rows(row - 1, 1), :] = value
        put(row, inside(row, jnp.maximum(value.astype(F32), 0.0)))

    conv_stage(2, join)
    conv_stage(3, hidden(2))
    norm_3 = take_stat(3)

    for row in range(height):
        value = joined[rows(row, 1), :].astype(F32) + normed(3, row + 1, norm_3)
        out_ref[rows(row, 1), :] = value.astype(BF16)

    end_halo(feature_halo())
    for k in range(3):
        end_halo(raw_halo(k))
    for k in range(4):
        pltpu.make_async_copy(peers.at[k], peers.at[k], stat_send.at[k]).wait()


def solution(mesh):
    imgs, strips = mesh.shape["img"], mesh.shape["row"]

    def on_device(tokens, proj_weight, proj_bias, conv_weight, bn_gain, bn_bias):
        images, height, cols, embed = tokens.shape
        convs, taps, _, width, _ = conv_weight.shape
        assert images == 1 and height % 2 == 0 and height >= 4
        count = imgs * strips
        assert strips % 2 == 0 and count == 2 ** (count.bit_length() - 1)
        cells = height * cols
        hbm = pl.BlockSpec(memory_space=pltpu.HBM)
        vmem = pl.BlockSpec(memory_space=pltpu.VMEM)
        operands = [
            tokens.reshape(cells, embed),
            proj_weight,
            proj_bias.reshape(1, width),
            conv_weight.reshape(convs * taps, taps * width, width),
            bn_gain,
            bn_bias,
        ]
        out = pl.pallas_call(
            functools.partial(kernel, imgs, strips, height, cols),
            out_shape=pltpu.VMEM((cells, width), BF16),
            in_specs=[hbm] * 6,
            out_specs=vmem,
            scratch_shapes=[
                pltpu.VMEM((cells, embed), BF16),
                pltpu.VMEM((embed, width), BF16),
                pltpu.VMEM((1, width), F32),
                pltpu.VMEM((convs * taps, taps * width, width), BF16),
                pltpu.VMEM((convs, width), F32),
                pltpu.VMEM((convs, width), F32),
                pltpu.VMEM((cells + 2 * cols, width), BF16),
                pltpu.VMEM((cells, width), BF16),
                pltpu.VMEM((cells + 2 * cols, taps * width), BF16),
                pltpu.VMEM((convs, cells, width), F32),
                pltpu.VMEM((convs - 1, 2, cols, width), BF16),
                pltpu.VMEM((convs - 1, 2, cols, width), BF16),
                pltpu.VMEM((convs, 2, width), F32),
                pltpu.VMEM((convs, count - 1, 2, width), F32),
                pltpu.SemaphoreType.DMA((7,)),
                pltpu.SemaphoreType.DMA((convs,)),
                pltpu.SemaphoreType.DMA((convs, 2)),
                pltpu.SemaphoreType.DMA((convs, 2)),
                pltpu.SemaphoreType.DMA((convs,)),
                pltpu.SemaphoreType.DMA((convs,)),
                pltpu.SemaphoreType.REGULAR,
                pltpu.SemaphoreType.REGULAR,
            ],
            compiler_params=pltpu.CompilerParams(
                collective_id=0, has_side_effects=True, vmem_limit_bytes=VMEM_LIMIT
            ),
        )(*[pltpu.with_memory_space_constraint(x, pltpu.HBM) for x in operands])
        return out.reshape(images, height, cols, width)

    in_specs = (P("img", "row", None, None), P(), P(), P(), P(), P())
    return jax.shard_map(
        on_device,
        mesh=mesh,
        in_specs=in_specs,
        out_specs=P("img", "row", None, None),
        check_vma=False,
    )
```

```python
import functools

import jax
import jax.numpy as jnp
from jax import lax
from jax.experimental import pallas as pl
from jax.experimental.pallas import tpu as pltpu
from jax.sharding import PartitionSpec as P

epsilon = 1e-05
LOGICAL = pl.DeviceIdType.LOGICAL
F32 = jnp.float32
BF16 = jnp.bfloat16
STEP = 1
EDGE = 16
UNROLL = 63
VMEM_LIMIT = 40 * 1024 * 1024


def bits_of(count):
    return [2**b for b in range(count.bit_length() - 1)]


def kernel(
    imgs,
    strips,
    height,
    cols,
    tokens_ref,
    pw_ref,
    pb_ref,
    cw_ref,
    gain_ref,
    bias_ref,
    out_ref,
    tok,
    pw,
    pb,
    cw,
    affine,
    feat,
    joined,
    xcat,
    raw,
    rim_out,
    rim_in,
    stats,
    peers,
    load_sem,
    weight_sem,
    halo_send,
    halo_recv,
    stat_send,
    stat_recv,
    near,
    everyone,
):
    count = imgs * strips
    width = feat.shape[-1]
    cells = height * cols
    me_row = lax.axis_index("row")
    me = lax.axis_index("img") * strips + me_row
    has_up, has_down = me_row > 0, me_row < strips - 1
    above = me - jnp.where(has_up, 1, 0)
    below = me + jnp.where(has_down, 1, 0)

    flips = [bit - 2 * bit * lax.rem(me // bit, 2) for bit in bits_of(count)]

    def peer(distance):
        if isinstance(distance, int):
            return me + sum(flip for b, flip in enumerate(flips) if distance >> b & 1)
        return me + sum(flip * lax.rem(distance // 2**b, 2) for b, flip in enumerate(flips))

    half = count // 2
    odd = lax.rem(me_row, 2)
    is_odd, is_even = odd == 1, odd == 0
    partner = me + 1 - 2 * odd

    def rows(first, number):
        return pl.ds(first * cols, number * cols)

    loads = [
        pltpu.make_async_copy(pw_ref, pw, load_sem.at[0]),
        pltpu.make_async_copy(tokens_ref.at[rows(0, 1)], tok.at[rows(0, 1)], load_sem.at[1]),
        pltpu.make_async_copy(
            tokens_ref.at[rows(height - 1, 1)], tok.at[rows(1, 1)], load_sem.at[1]
        ),
        pltpu.make_async_copy(pb_ref, pb, load_sem.at[2]),
        pltpu.make_async_copy(
            tokens_ref.at[rows(1, height - 2)], tok.at[rows(2, height - 2)], load_sem.at[3]
        ),
        pltpu.make_async_copy(gain_ref, affine.at[0], load_sem.at[4]),
        pltpu.make_async_copy(bias_ref, affine.at[1], load_sem.at[4]),
    ]
    rims = pltpu.make_async_copy(tok.at[rows(0, 2)], tok.at[rows(0, 2)], load_sem.at[1])
    affines = pltpu.make_async_copy(affine, affine, load_sem.at[4])
    weights = [
        pltpu.make_async_copy(cw_ref.at[at], cw.at[at], weight_sem.at[i])
        for i, at in enumerate((pl.ds(0, 3), pl.ds(3, 9)))
    ]
    for load in loads[:4]:
        load.start()

    barrier = pltpu.get_barrier_semaphore()

    def greet(device):
        pl.semaphore_signal(barrier, inc=1, device_id=device, device_id_type=LOGICAL)

    @pl.when(is_odd)
    def _():
        greet(partner)

        @pl.when(has_down)
        def _():
            greet(below)

    @pl.when(jnp.logical_and(is_even, me_row >= 2))
    def _():
        greet(me - 2)

    @pl.loop(1, half)
    def _(distance):
        greet(peer(2 * (half - distance)) + 1 - odd)

    @pl.when(is_even)
    def _():
        greet(partner)

    loads[4].start(priority=1)
    for weight in weights:
        weight.start(priority=1)
    for load in loads[5:]:
        load.start(priority=1)

    @pl.when(jnp.logical_not(has_up))
    def _():
        feat[rows(0, 1), :] = jnp.zeros((cols, width), BF16)
        for k in range(3):
            rim_in[k, 0] = jnp.zeros((cols, width), BF16)

    @pl.when(jnp.logical_not(has_down))
    def _():
        feat[rows(height + 1, 1), :] = jnp.zeros((cols, width), BF16)
        for k in range(3):
            rim_in[k, 1] = jnp.zeros((cols, width), BF16)

    column = lax.broadcasted_iota(jnp.int32, (EDGE, width), 0)
    at_left, at_right = column == 0, column == EDGE - 1
    left, centre, right = (slice(i * width, (i + 1) * width) for i in range(3))

    def put(row, value):
        first, last = row * cols, row * cols + cols - EDGE
        before, after = pltpu.roll(value, 1, 0), pltpu.roll(value, cols - 1, 0)
        xcat[pl.ds(first, EDGE), left] = jnp.where(at_left, 0.0, before[:EDGE]).astype(BF16)
        xcat[pl.ds(first + EDGE, cols - EDGE), left] = before[EDGE:].astype(BF16)
        xcat[rows(row, 1), centre] = value.astype(BF16)
        xcat[pl.ds(first, cols - EDGE), right] = after[:-EDGE].astype(BF16)
        xcat[pl.ds(last, EDGE), right] = jnp.where(at_right, 0.0, after[-EDGE:]).astype(BF16)

    def project(slot, number, where):
        value = jnp.dot(tok[rows(slot, number), :], pw[...], preferred_element_type=F32)
        value = (value + pb[...]).astype(BF16)
        for i, row in enumerate(where):
            feat[rows(row + 1, 1), :] = value[i * cols : (i + 1) * cols]

    def activate(row):
        put(row, jnp.maximum(feat[rows(row, 1), :].astype(F32), 0.0))

    def halo(phase, up_from, up_to, down_from, down_to):
        up = pltpu.make_async_remote_copy(
            src_ref=up_from,
            dst_ref=up_to,
            send_sem=halo_send.at[0],
            recv_sem=halo_recv.at[phase % 2, 1],
            device_id=above,
            device_id_type=LOGICAL,
        )
        down = pltpu.make_async_remote_copy(
            src_ref=down_from,
            dst_ref=down_to,
            send_sem=halo_send.at[1],
            recv_sem=halo_recv.at[phase % 2, 0],
            device_id=below,
            device_id_type=LOGICAL,
        )
        return up, down

    def feature_halo():
        return halo(
            0,
            feat.at[rows(1, 1)],
            feat.at[rows(height + 1, 1)],
            feat.at[rows(height, 1)],
            feat.at[rows(0, 1)],
        )

    def raw_halo(k):
        return halo(
            k + 1, rim_out.at[k, 0], rim_in.at[k, 1], rim_out.at[k, 1], rim_in.at[k, 0]
        )

    def send_halo(pair):
        up, down = pair

        @pl.when(has_up)
        def _():
            up.start()

        @pl.when(has_down)
        def _():
            down.start()

    def take_halo(pair):
        up, down = pair

        @pl.when(has_up)
        def _():
            down.wait_recv()

        @pl.when(has_down)
        def _():
            up.wait_recv()

    def end_halos():
        for side, there in enumerate((has_up, has_down)):

            @pl.when(there)
            def _():
                four = feat.at[rows(0, 4)]
                pltpu.make_async_copy(four, four, halo_send.at[side]).wait()

    def taps(k, first, number, which):
        return sum(
            jnp.dot(xcat[rows(first + dy, number), :], cw[3 * k + dy], preferred_element_type=F32)
            for dy in which
        )

    def fold(value):
        return jnp.sum(value.reshape(value.shape[0] // 8, 8, width), axis=0)

    class Moments:
        def add(self, value):
            if not hasattr(self, "pivot"):
                self.pivot = jnp.sum(fold(value), axis=0, keepdims=True) / value.shape[0]
                self.first = jnp.zeros((8, width), F32)
                self.second = jnp.zeros((8, width), F32)
            gap = value - self.pivot
            self.first += fold(gap)
            self.second += fold(jnp.square(gap))

        def total(self):
            first = jnp.sum(self.first, axis=0, keepdims=True)
            second = jnp.sum(self.second, axis=0, keepdims=True)
            return first + cells * self.pivot, second - jnp.square(first) / cells

    def stat_copy(k, distance):
        return pltpu.make_async_remote_copy(
            src_ref=stats.at[k],
            dst_ref=peers.at[k, distance - 1],
            send_sem=stat_send,
            recv_sem=stat_recv.at[k % 2],
            device_id=peer(distance),
            device_id_type=LOGICAL,
        )

    def send_stat(k, moments):
        total, squares = moments.total()
        stats[k] = jnp.concatenate([total, squares], axis=0)
        if count - 1 <= UNROLL:
            for distance in range(count - 1, 0, -1):
                stat_copy(k, distance).start()
        else:
            pl.loop(1, count)(lambda distance: stat_copy(k, count - distance).start())

    def take_stat(k):
        own = stats[k]
        pltpu.make_async_copy(peers.at[k], peers.at[k], stat_recv.at[k % 2]).wait()
        every = peers[k]
        total = jnp.sum(every, axis=0) + own
        even = total[0:1] / count
        gaps = jnp.sum(jnp.square(every[:, 0, :] - even), axis=0, keepdims=True)
        gaps += jnp.square(own[0:1] - even)
        squares = total[1:2] + gaps / cells
        size = cells * count
        average = total[0:1] / size
        scale = lax.rsqrt(squares / size + epsilon) * affine[0, k : k + 1, :]
        return scale, affine[1, k : k + 1, :] - average * scale

    def normed(k, row, norm):
        scale, shift = norm
        if row == 0:
            value = rim_in[k, 0].astype(F32)
        elif row == height + 1:
            value = rim_in[k, 1].astype(F32)
        else:
            value = raw[k, rows(row - 1, 1), :]
        return value * scale + shift

    def inside(row, value):
        if row == 0:
            return jnp.where(has_up, value, 0.0)
        if row == height + 1:
            return jnp.where(has_down, value, 0.0)
        return value

    def conv_stage(k, fill):
        moments = Moments()
        filled = 0
        for first in range(0, height, STEP):
            while filled < first + STEP + 2:
                fill(filled)
                filled += 1
            value = taps(k, first, STEP, range(3))
            raw[k, rows(first, STEP), :] = value
            if k < 3 and first == 0:
                rim_out[k, 0] = value[:cols].astype(BF16)
            if k < 3 and first + STEP == height:
                rim_out[k, 1] = value[-cols:].astype(BF16)
            moments.add(value)
        send_stat(k, moments)
        if k < 3:
            send_halo(raw_halo(k))

    loads[0].wait()
    rims.wait()
    loads[3].wait()
    project(0, 1, (0,))
    project(1, 1, (height - 1,))

    @pl.when(is_even)
    def _():
        beside = jnp.where(me_row >= 2, 1, 0) + jnp.where(me_row + 2 < strips, 1, 0)
        pl.semaphore_wait(barrier, 1 + beside)
        pl.semaphore_signal(near, inc=1, device_id=partner, device_id_type=LOGICAL)

    @pl.when(is_odd)
    def _():
        pl.semaphore_wait(near, 1)

    send_halo(feature_halo())
    loads[4].wait()
    activate(1)
    activate(height)
    half_rows = (height - 2) // 2
    for slot in (2, 2 + half_rows):
        project(slot, half_rows, range(slot - 1, slot - 1 + half_rows))
        for row in range(slot, slot + half_rows):
            activate(row)

    weights[0].wait()
    moments = Moments()
    for first in (1, 1 + half_rows):
        value = taps(0, first, half_rows, range(3))
        raw[0, rows(first, half_rows), :] = value
        moments.add(value)
    top = taps(0, 0, 1, (1, 2))
    bottom = taps(0, height - 1, 1, (0, 1))
    raw[0, rows(0, 1), :] = top
    raw[0, rows(height - 1, 1), :] = bottom
    take_halo(feature_halo())
    activate(0)
    activate(height + 1)
    top = raw[0, rows(0, 1), :] + taps(0, 0, 1, (0,))
    bottom = raw[0, rows(height - 1, 1), :] + taps(0, height - 1, 1, (2,))
    for side, row, value in ((0, 0, top), (1, height - 1, bottom)):
        raw[0, rows(row, 1), :] = value
        rim_out[0, side] = value.astype(BF16)
        moments.add(value)

    @pl.when(is_odd)
    def _():
        pl.semaphore_wait(barrier, count - 1)
        pl.semaphore_signal(everyone, inc=1, device_id=partner, device_id_type=LOGICAL)

    @pl.when(is_even)
    def _():
        pl.semaphore_wait(everyone, 1)

    send_stat(0, moments)
    send_halo(raw_halo(0))
    affines.wait()
    weights[1].wait()

    def hidden(k):
        norm = take_stat(k)
        take_halo(raw_halo(k))

        def fill(row):
            put(row, inside(row, jnp.maximum(normed(k, row, norm), 0.0)))

        return fill

    conv_stage(1, hidden(0))

    norm_1 = take_stat(1)
    take_halo(raw_halo(1))

    def join(row):
        value = (feat[rows(row, 1), :].astype(F32) + normed(1, row, norm_1)).astype(BF16)
        if 1 <= row <= height:
            joined[rows(row - 1, 1), :] = value
        put(row, inside(row, jnp.maximum(value.astype(F32), 0.0)))

    conv_stage(2, join)
    conv_stage(3, hidden(2))
    norm_3 = take_stat(3)

    for row in range(height):
        value = joined[rows(row, 1), :].astype(F32) + normed(3, row + 1, norm_3)
        out_ref[rows(row, 1), :] = value.astype(BF16)

    end_halos()
    pltpu.make_async_copy(peers, peers, stat_send).wait()


def solution(mesh):
    imgs, strips = mesh.shape["img"], mesh.shape["row"]

    def on_device(tokens, proj_weight, proj_bias, conv_weight, bn_gain, bn_bias):
        images, height, cols, embed = tokens.shape
        convs, taps, _, width, _ = conv_weight.shape
        assert images == 1 and height % 2 == 0 and height >= 4
        count = imgs * strips
        assert strips % 2 == 0 and count == 2 ** (count.bit_length() - 1)
        cells = height * cols
        hbm = pl.BlockSpec(memory_space=pltpu.HBM)
        vmem = pl.BlockSpec(memory_space=pltpu.VMEM)
        operands = [
            tokens.reshape(cells, embed),
            proj_weight,
            proj_bias.reshape(1, width),
            conv_weight.reshape(convs * taps, taps * width, width),
            bn_gain,
            bn_bias,
        ]
        out = pl.pallas_call(
            functools.partial(kernel, imgs, strips, height, cols),
            out_shape=pltpu.VMEM((cells, width), BF16),
            in_specs=[hbm] * 6,
            out_specs=vmem,
            scratch_shapes=[
                pltpu.VMEM((cells, embed), BF16),
                pltpu.VMEM((embed, width), BF16),
                pltpu.VMEM((1, width), F32),
                pltpu.VMEM((convs * taps, taps * width, width), BF16),
                pltpu.VMEM((2, convs, width), F32),
                pltpu.VMEM((cells + 2 * cols, width), BF16),
                pltpu.VMEM((cells, width), BF16),
                pltpu.VMEM((cells + 2 * cols, taps * width), BF16),
                pltpu.VMEM((convs, cells, width), F32),
                pltpu.VMEM((convs - 1, 2, cols, width), BF16),
                pltpu.VMEM((convs - 1, 2, cols, width), BF16),
                pltpu.VMEM((convs, 2, width), F32),
                pltpu.VMEM((convs, count - 1, 2, width), F32),
                pltpu.SemaphoreType.DMA((5,)),
                pltpu.SemaphoreType.DMA((2,)),
                pltpu.SemaphoreType.DMA((2,)),
                pltpu.SemaphoreType.DMA((2, 2)),
                pltpu.SemaphoreType.DMA,
                pltpu.SemaphoreType.DMA((2,)),
                pltpu.SemaphoreType.REGULAR,
                pltpu.SemaphoreType.REGULAR,
            ],
            compiler_params=pltpu.CompilerParams(
                collective_id=0, has_side_effects=True, vmem_limit_bytes=VMEM_LIMIT
            ),
        )(*[pltpu.with_memory_space_constraint(x, pltpu.HBM) for x in operands])
        return out.reshape(images, height, cols, width)

    in_specs = (P("img", "row", None, None), P(), P(), P(), P(), P())
    return jax.shard_map(
        on_device,
        mesh=mesh,
        in_specs=in_specs,
        out_specs=P("img", "row", None, None),
        check_vma=False,
    )
```

```python
import functools

import jax
import jax.numpy as jnp
from jax import lax
from jax.experimental import pallas as pl
from jax.experimental.pallas import tpu as pltpu
from jax.sharding import PartitionSpec as P

epsilon = 1e-05
LOGICAL = pl.DeviceIdType.LOGICAL
F32 = jnp.float32
BF16 = jnp.bfloat16
STEP = 1
LANES = 128
EDGE = 16
UNROLL = 63
VMEM_LIMIT = 40 * 1024 * 1024


def bits_of(count):
    return [2**b for b in range(count.bit_length() - 1)]


def kernel(
    imgs,
    strips,
    height,
    cols,
    tokens_ref,
    pw_ref,
    pb_ref,
    cw_ref,
    gain_ref,
    bias_ref,
    out_ref,
    tok,
    pw,
    pb,
    cw,
    affine,
    feat,
    joined,
    xcat,
    raw,
    rim_out,
    rim_in,
    stats,
    peers,
    load_sem,
    weight_sem,
    halo_send,
    halo_recv,
    stat_send,
    stat_recv,
    near,
    everyone,
):
    count = imgs * strips
    width = feat.shape[-1]
    cells = height * cols
    me_row = lax.axis_index("row")
    me = lax.axis_index("img") * strips + me_row
    has_up, has_down = me_row > 0, me_row < strips - 1
    above = me - jnp.where(has_up, 1, 0)
    below = me + jnp.where(has_down, 1, 0)

    flips = [bit - 2 * bit * lax.rem(me // bit, 2) for bit in bits_of(count)]

    def peer(distance):
        if isinstance(distance, int):
            return me + sum(flip for b, flip in enumerate(flips) if distance >> b & 1)
        return me + sum(flip * lax.rem(distance // 2**b, 2) for b, flip in enumerate(flips))

    half = count // 2
    odd = lax.rem(me_row, 2)
    is_odd, is_even = odd == 1, odd == 0
    partner = me + 1 - 2 * odd

    def rows(first, number):
        return pl.ds(first * cols, number * cols)

    loads = [
        pltpu.make_async_copy(pw_ref, pw, load_sem.at[0]),
        pltpu.make_async_copy(tokens_ref.at[rows(0, 1)], tok.at[rows(0, 1)], load_sem.at[1]),
        pltpu.make_async_copy(
            tokens_ref.at[rows(height - 1, 1)], tok.at[rows(1, 1)], load_sem.at[1]
        ),
        pltpu.make_async_copy(pb_ref, pb, load_sem.at[2]),
        pltpu.make_async_copy(
            tokens_ref.at[rows(1, height - 2)], tok.at[rows(2, height - 2)], load_sem.at[3]
        ),
        pltpu.make_async_copy(gain_ref, affine.at[0], load_sem.at[4]),
        pltpu.make_async_copy(bias_ref, affine.at[1], load_sem.at[4]),
    ]
    rims = pltpu.make_async_copy(tok.at[rows(0, 2)], tok.at[rows(0, 2)], load_sem.at[1])
    affines = pltpu.make_async_copy(affine, affine, load_sem.at[4])
    weights = [
        pltpu.make_async_copy(cw_ref.at[at], cw.at[at], weight_sem.at[i])
        for i, at in enumerate((pl.ds(0, 3), pl.ds(3, 9)))
    ]
    for load in loads[:4]:
        load.start()

    barrier = pltpu.get_barrier_semaphore()

    def greet(device):
        pl.semaphore_signal(barrier, inc=1, device_id=device, device_id_type=LOGICAL)

    @pl.when(is_odd)
    def _():
        greet(partner)

        @pl.when(has_down)
        def _():
            greet(below)

    @pl.when(jnp.logical_and(is_even, me_row >= 2))
    def _():
        greet(me - 2)

    @pl.loop(1, half)
    def _(distance):
        greet(peer(2 * (half - distance)) + 1 - odd)

    @pl.when(is_even)
    def _():
        greet(partner)

    loads[4].start(priority=1)
    for weight in weights:
        weight.start(priority=1)
    for load in loads[5:]:
        load.start(priority=1)

    @pl.when(jnp.logical_not(has_up))
    def _():
        feat[rows(0, 1), :] = jnp.zeros((cols, width), BF16)
        for k in range(3):
            rim_in[k, 0] = jnp.zeros((cols, width), BF16)

    @pl.when(jnp.logical_not(has_down))
    def _():
        feat[rows(height + 1, 1), :] = jnp.zeros((cols, width), BF16)
        for k in range(3):
            rim_in[k, 1] = jnp.zeros((cols, width), BF16)

    column = lax.broadcasted_iota(jnp.int32, (EDGE, width), 0)
    at_left, at_right = column == 0, column == EDGE - 1
    left, centre, right = (slice(i * width, (i + 1) * width) for i in range(3))

    def put(row, value):
        first, last = row * cols, row * cols + cols - EDGE
        before, after = pltpu.roll(value, 1, 0), pltpu.roll(value, cols - 1, 0)
        xcat[pl.ds(first, EDGE), left] = jnp.where(at_left, 0.0, before[:EDGE]).astype(BF16)
        xcat[pl.ds(first + EDGE, cols - EDGE), left] = before[EDGE:].astype(BF16)
        xcat[rows(row, 1), centre] = value.astype(BF16)
        xcat[pl.ds(first, cols - EDGE), right] = after[:-EDGE].astype(BF16)
        xcat[pl.ds(last, EDGE), right] = jnp.where(at_right, 0.0, after[-EDGE:]).astype(BF16)

    def project(slot, number, where):
        value = jnp.dot(tok[rows(slot, number), :], pw[...], preferred_element_type=F32)
        value = (value + pb[...]).astype(BF16)
        for i, row in enumerate(where):
            feat[rows(row + 1, 1), :] = value[i * cols : (i + 1) * cols]

    def activate(row):
        put(row, jnp.maximum(feat[rows(row, 1), :].astype(F32), 0.0))

    def halo(phase, up_from, up_to, down_from, down_to):
        up = pltpu.make_async_remote_copy(
            src_ref=up_from,
            dst_ref=up_to,
            send_sem=halo_send.at[0],
            recv_sem=halo_recv.at[phase % 2, 1],
            device_id=above,
            device_id_type=LOGICAL,
        )
        down = pltpu.make_async_remote_copy(
            src_ref=down_from,
            dst_ref=down_to,
            send_sem=halo_send.at[1],
            recv_sem=halo_recv.at[phase % 2, 0],
            device_id=below,
            device_id_type=LOGICAL,
        )
        return up, down

    def feature_halo():
        return halo(
            0,
            feat.at[rows(1, 1)],
            feat.at[rows(height + 1, 1)],
            feat.at[rows(height, 1)],
            feat.at[rows(0, 1)],
        )

    def raw_halo(k):
        return halo(
            k + 1, rim_out.at[k, 0], rim_in.at[k, 1], rim_out.at[k, 1], rim_in.at[k, 0]
        )

    def send_halo(pair):
        up, down = pair

        @pl.when(has_up)
        def _():
            up.start()

        @pl.when(has_down)
        def _():
            down.start()

    def take_halo(pair):
        up, down = pair

        @pl.when(has_up)
        def _():
            down.wait_recv()

        @pl.when(has_down)
        def _():
            up.wait_recv()

    def end_halos():
        for side, there in enumerate((has_up, has_down)):

            @pl.when(there)
            def _():
                four = feat.at[rows(0, 4)]
                pltpu.make_async_copy(four, four, halo_send.at[side]).wait()

    def taps(k, first, number, which):
        return sum(
            jnp.dot(xcat[rows(first + dy, number), :], cw[3 * k + dy], preferred_element_type=F32)
            for dy in which
        )

    def fold(value):
        return jnp.sum(value.reshape(value.shape[0] // 8, 8, width), axis=0)

    class Moments:
        def add(self, value):
            if not hasattr(self, "pivot"):
                self.pivot = jnp.sum(fold(value), axis=0, keepdims=True) / value.shape[0]
                self.first = jnp.zeros((8, width), F32)
                self.second = jnp.zeros((8, width), F32)
            gap = value - self.pivot
            self.first += fold(gap)
            self.second += fold(jnp.square(gap))

        def total(self):
            first = jnp.sum(self.first, axis=0, keepdims=True)
            second = jnp.sum(self.second, axis=0, keepdims=True)
            return first + cells * self.pivot, second - jnp.square(first) / cells

    parts = width // LANES

    def split(row):
        return [row[:, i * LANES : (i + 1) * LANES] for i in range(parts)]

    def joint(value):
        return jnp.concatenate([value[i : i + 1] for i in range(parts)], axis=1)

    def stat_copy(k, distance):
        return pltpu.make_async_remote_copy(
            src_ref=stats.at[k],
            dst_ref=peers.at[k, distance - 1],
            send_sem=stat_send,
            recv_sem=stat_recv.at[k % 2],
            device_id=peer(distance),
            device_id_type=LOGICAL,
        )

    def reach(distance):
        far = distance // strips
        return far // 2 + far % 2 + distance % strips // 2, 1 - distance % 2

    def send_stat(k, moments):
        total, squares = moments.total()
        stats[k] = jnp.concatenate(split(total) + split(squares), axis=0)
        if count - 1 <= UNROLL:
            for distance in sorted(range(1, count), key=reach, reverse=True):
                stat_copy(k, distance).start()
        else:
            pl.loop(1, count)(lambda distance: stat_copy(k, count - distance).start())

    def take_stat(k):
        own = stats[k]
        pltpu.make_async_copy(peers.at[k], peers.at[k], stat_recv.at[k % 2]).wait()
        every = peers[k]
        total = jnp.sum(every, axis=0) + own
        even = total[:parts] / count
        gaps = jnp.sum(jnp.square(every[:, :parts, :] - even), axis=0)
        gaps += jnp.square(own[:parts] - even)
        squares = total[parts:] + gaps / cells
        size = cells * count
        average = joint(total[:parts] / size)
        scale = joint(lax.rsqrt(squares / size + epsilon)) * affine[0, k : k + 1, :]
        return scale, affine[1, k : k + 1, :] - average * scale

    def normed(k, row, norm):
        scale, shift = norm
        if row == 0:
            value = rim_in[k, 0].astype(F32)
        elif row == height + 1:
            value = rim_in[k, 1].astype(F32)
        else:
            value = raw[k, rows(row - 1, 1), :]
        return value * scale + shift

    def inside(row, value):
        if row == 0:
            return jnp.where(has_up, value, 0.0)
        if row == height + 1:
            return jnp.where(has_down, value, 0.0)
        return value

    def conv_stage(k, fill):
        moments = Moments()
        filled = 0
        for first in range(0, height, STEP):
            while filled < first + STEP + 2:
                fill(filled)
                filled += 1
            value = taps(k, first, STEP, range(3))
            raw[k, rows(first, STEP), :] = value
            if k < 3 and first == 0:
                rim_out[k, 0] = value[:cols].astype(BF16)
            if k < 3 and first + STEP == height:
                rim_out[k, 1] = value[-cols:].astype(BF16)
            moments.add(value)
        send_stat(k, moments)
        if k < 3:
            send_halo(raw_halo(k))

    loads[0].wait()
    rims.wait()
    loads[3].wait()
    project(0, 1, (0,))
    project(1, 1, (height - 1,))

    @pl.when(is_even)
    def _():
        beside = jnp.where(me_row >= 2, 1, 0) + jnp.where(me_row + 2 < strips, 1, 0)
        pl.semaphore_wait(barrier, 1 + beside)
        pl.semaphore_signal(near, inc=1, device_id=partner, device_id_type=LOGICAL)

    @pl.when(is_odd)
    def _():
        pl.semaphore_wait(near, 1)

    send_halo(feature_halo())
    loads[4].wait()
    activate(1)
    activate(height)
    half_rows = (height - 2) // 2
    for slot in (2, 2 + half_rows):
        project(slot, half_rows, range(slot - 1, slot - 1 + half_rows))
        for row in range(slot, slot + half_rows):
            activate(row)

    weights[0].wait()
    moments = Moments()
    for first in range(1, height - 1):
        value = taps(0, first, 1, range(3))
        raw[0, rows(first, 1), :] = value
        moments.add(value)
    top = taps(0, 0, 1, (1, 2))
    bottom = taps(0, height - 1, 1, (0, 1))
    raw[0, rows(0, 1), :] = top
    raw[0, rows(height - 1, 1), :] = bottom
    take_halo(feature_halo())
    activate(0)
    activate(height + 1)
    top = raw[0, rows(0, 1), :] + taps(0, 0, 1, (0,))
    bottom = raw[0, rows(height - 1, 1), :] + taps(0, height - 1, 1, (2,))
    for side, row, value in ((0, 0, top), (1, height - 1, bottom)):
        raw[0, rows(row, 1), :] = value
        rim_out[0, side] = value.astype(BF16)
        moments.add(value)

    @pl.when(is_odd)
    def _():
        pl.semaphore_wait(barrier, count - 1)
        pl.semaphore_signal(everyone, inc=1, device_id=partner, device_id_type=LOGICAL)

    @pl.when(is_even)
    def _():
        pl.semaphore_wait(everyone, 1)

    send_stat(0, moments)
    send_halo(raw_halo(0))
    affines.wait()
    weights[1].wait()

    def hidden(k):
        norm = take_stat(k)
        take_halo(raw_halo(k))

        def fill(row):
            put(row, inside(row, jnp.maximum(normed(k, row, norm), 0.0)))

        return fill

    conv_stage(1, hidden(0))

    norm_1 = take_stat(1)
    take_halo(raw_halo(1))

    def join(row):
        value = (feat[rows(row, 1), :].astype(F32) + normed(1, row, norm_1)).astype(BF16)
        if 1 <= row <= height:
            joined[rows(row - 1, 1), :] = value
        put(row, inside(row, jnp.maximum(value.astype(F32), 0.0)))

    conv_stage(2, join)
    conv_stage(3, hidden(2))
    norm_3 = take_stat(3)

    for row in range(height):
        value = joined[rows(row, 1), :].astype(F32) + normed(3, row + 1, norm_3)
        out_ref[rows(row, 1), :] = value.astype(BF16)

    end_halos()
    pltpu.make_async_copy(peers, peers, stat_send).wait()


def solution(mesh):
    imgs, strips = mesh.shape["img"], mesh.shape["row"]

    def on_device(tokens, proj_weight, proj_bias, conv_weight, bn_gain, bn_bias):
        images, height, cols, embed = tokens.shape
        convs, taps, _, width, _ = conv_weight.shape
        assert images == 1 and height % 2 == 0 and height >= 4
        count = imgs * strips
        assert strips % 2 == 0 and count == 2 ** (count.bit_length() - 1)
        cells = height * cols
        hbm = pl.BlockSpec(memory_space=pltpu.HBM)
        vmem = pl.BlockSpec(memory_space=pltpu.VMEM)
        operands = [
            tokens.reshape(cells, embed),
            proj_weight,
            proj_bias.reshape(1, width),
            conv_weight.reshape(convs * taps, taps * width, width),
            bn_gain,
            bn_bias,
        ]
        out = pl.pallas_call(
            functools.partial(kernel, imgs, strips, height, cols),
            out_shape=pltpu.VMEM((cells, width), BF16),
            in_specs=[hbm] * 6,
            out_specs=vmem,
            scratch_shapes=[
                pltpu.VMEM((cells, embed), BF16),
                pltpu.VMEM((embed, width), BF16),
                pltpu.VMEM((1, width), F32),
                pltpu.VMEM((convs * taps, taps * width, width), BF16),
                pltpu.VMEM((2, convs, width), F32),
                pltpu.VMEM((cells + 2 * cols, width), BF16),
                pltpu.VMEM((cells, width), BF16),
                pltpu.VMEM((cells + 2 * cols, taps * width), BF16),
                pltpu.VMEM((convs, cells, width), F32),
                pltpu.VMEM((convs - 1, 2, cols, width), BF16),
                pltpu.VMEM((convs - 1, 2, cols, width), BF16),
                pltpu.VMEM((convs, 2 * width // LANES, LANES), F32),
                pltpu.VMEM((convs, count - 1, 2 * width // LANES, LANES), F32),
                pltpu.SemaphoreType.DMA((5,)),
                pltpu.SemaphoreType.DMA((2,)),
                pltpu.SemaphoreType.DMA((2,)),
                pltpu.SemaphoreType.DMA((2, 2)),
                pltpu.SemaphoreType.DMA,
                pltpu.SemaphoreType.DMA((2,)),
                pltpu.SemaphoreType.REGULAR,
                pltpu.SemaphoreType.REGULAR,
            ],
            compiler_params=pltpu.CompilerParams(
                collective_id=0, has_side_effects=True, vmem_limit_bytes=VMEM_LIMIT
            ),
        )(*[pltpu.with_memory_space_constraint(x, pltpu.HBM) for x in operands])
        return out.reshape(images, height, cols, width)

    in_specs = (P("img", "row", None, None), P(), P(), P(), P(), P())
    return jax.shard_map(
        on_device,
        mesh=mesh,
        in_specs=in_specs,
        out_specs=P("img", "row", None, None),
        check_vma=False,
    )
```
